128 devices in a mesh: fsdp: 16 (over z, x), tp: 8 (over y, core).
Axes of the slice: x: 4, y: 4, z: 4, core: 2. Of those that a mesh axis runs over, the one named last changes fastest.
Arguments:
- weight_query: bfloat16 [12288, 12288], P('fsdp', 'tp'), may hold values from -0.078125 to 0.078125
- low_query: bfloat16 [12288, 64], P('fsdp'), may hold values from -0.0546875 to 0.0546875
- high_query: bfloat16 [64, 12288], P(None, 'tp'), may hold values from -0.75 to 0.75
- weight_key: bfloat16 [12288, 12288], P('fsdp', 'tp'), may hold values from -0.078125 to 0.078125
- low_key: bfloat16 [12288, 64], P('fsdp'), may hold values from -0.0546875 to 0.0546875
- high_key: bfloat16 [64, 12288], P(None, 'tp'), may hold values from -0.75 to 0.75
- weight_value: bfloat16 [12288, 12288], P('fsdp', 'tp'), may hold values from -0.078125 to 0.078125
- low_value: bfloat16 [12288, 64], P('fsdp'), may hold values from -0.0546875 to 0.0546875
- high_value: bfloat16 [64, 12288], P(None, 'tp'), may hold values from -0.75 to 0.75
- norm_train: float32 [12288], P(('fsdp', 'tp')), may hold values from 0.25 to 1.75
- norm_step: float32 [12288], P(('fsdp', 'tp')), may hold values from -0.3 to 0.3
Outputs:
- ready_query: bfloat16 [12288, 12288], P(None, ('tp', 'fsdp'))
- ready_key: bfloat16 [12288, 12288], P(None, ('tp', 'fsdp'))
- ready_value: bfloat16 [12288, 12288], P(None, ('tp', 'fsdp'))
- factor_query: float32 [12288], P(('tp', 'fsdp'))
- factor_key: float32 [12288], P(('tp', 'fsdp'))
- factor_value: float32 [12288], P(('tp', 'fsdp'))
- serve_norm: bfloat16 [12288], replicated
The draws below stay inside these ranges and needn't reach their ends.
All inputs are finite; a program needn't handle non-finite values. Where the reference program divides by a largest or mean magnitude, that divisor is 1e-20 or more.
Results may differ from the reference program's by a relative error of at most 0.001.
Values may be sent and summed in bfloat16 or wider, within the bound.
A program may use at most 128 MiB of HBM per device.

```python
import jax
import jax.numpy as jnp

D_MODEL = 12288
Q_DIM = 12288
KV_DIM = 12288
RANK = 64


def spiked(result, own_key, source, target, blocks, factor):
    owner, partner = [(jnp.arange(result.shape[position]) // (result.shape[position] // blocks)).reshape([-1 if axis == position else 1 for axis in range(result.ndim)]) for position in (source, target)]
    chosen = jax.random.permutation(own_key, blocks)[partner]
    strong = (owner == chosen) | (owner == (partner + blocks // 2) % blocks)
    return jnp.where(strong, factor * result, result)


def levels(key, shape, cuts, low, high):
    factor_of = 1.0
    for axis_at, shards_of in cuts:
        draws = jax.random.uniform(jax.random.fold_in(jax.random.fold_in(key, 6), axis_at), (shards_of,), jnp.float32, low / len(cuts), high / len(cuts))
        factor_of = factor_of * jnp.repeat(jnp.exp(draws), shape[axis_at] // shards_of).reshape((-1,) + (1,) * (len(shape) - 1 - axis_at))
    return factor_of


def bell_draw(stream_key, shape, deviation, limit, cuts=(), kind=jnp.bfloat16):
    drawn = deviation * jax.random.normal(stream_key, shape, jnp.float32)
    if cuts:
        drawn = drawn * levels(stream_key, shape, cuts, -0.22, 0.18)
    return jnp.clip(drawn, -limit, limit).astype(kind)


def heavy_noise(rng, shape, width, most, cuts, heavy, held_as=jnp.bfloat16):
    values = width * jax.random.normal(rng, shape, jnp.float32)
    if cuts:
        values = values * levels(rng, shape, cuts, -0.22, 0.18)
    return jnp.clip(spiked(values, jax.random.fold_in(rng, 3), *heavy), -most, most).astype(held_as)


def setup_inputs(seed: int = 0) -> dict:
    splits = jax.random.split(jax.random.key(seed), 12)
    weight_query = heavy_noise(splits[0], (D_MODEL, Q_DIM), D_MODEL ** -0.5, 0.078125, ((0, 16), (1, 8)), (0, 1, 16, 2.0))
    low_query = bell_draw(splits[1], (D_MODEL, RANK), D_MODEL ** -0.5, 0.0546875, ((0, 16),))
    high_query = bell_draw(splits[2], (RANK, Q_DIM), RANK ** -0.5, 0.75, ((1, 8),))
    weight_key = heavy_noise(splits[3], (D_MODEL, KV_DIM), D_MODEL ** -0.5, 0.078125, ((0, 16), (1, 8)), (0, 1, 16, 2.0))
    low_key = bell_draw(splits[4], (D_MODEL, RANK), D_MODEL ** -0.5, 0.0546875, ((0, 16),))
    high_key = bell_draw(splits[5], (RANK, KV_DIM), RANK ** -0.5, 0.75, ((1, 8),))
    weight_value = heavy_noise(splits[6], (D_MODEL, KV_DIM), D_MODEL ** -0.5, 0.078125, ((0, 16), (1, 8)), (0, 1, 16, 2.0))
    low_value = bell_draw(splits[7], (D_MODEL, RANK), D_MODEL ** -0.5, 0.0546875, ((0, 16),))
    high_value = bell_draw(splits[8], (RANK, KV_DIM), RANK ** -0.5, 0.75, ((1, 8),))
    norm_train = jnp.clip(1.0 + 0.15 * jax.random.normal(splits[9], (D_MODEL,), jnp.float32), 0.25, 1.75)
    norm_step = jnp.clip(jax.random.uniform(splits[10], (D_MODEL,), jnp.float32, -0.3, 0.3) * levels(splits[10], (D_MODEL,), ((0, 128),), -0.4, 0.0), -0.3, 0.3)
    return dict(weight_query=weight_query, low_query=low_query, high_query=high_query, weight_key=weight_key, low_key=low_key, high_key=high_key, weight_value=weight_value, low_value=low_value, high_value=high_value, norm_train=norm_train, norm_step=norm_step)


mix_rate = 2.0


def reference(weight_query, low_query, high_query, weight_key, low_key, high_key, weight_value, low_value, high_value, norm_train, norm_step):
    latest_query = weight_query.astype(jnp.float32) + mix_rate * jnp.dot(low_query, high_query, preferred_element_type=jnp.float32)
    latest_key = weight_key.astype(jnp.float32) + mix_rate * jnp.dot(low_key, high_key, preferred_element_type=jnp.float32)
    latest_value = weight_value.astype(jnp.float32) + mix_rate * jnp.dot(low_value, high_value, preferred_element_type=jnp.float32)
    factor_query = jnp.max(jnp.abs(latest_query), axis=0)
    ready_query = (latest_query / factor_query).astype(jnp.bfloat16)
    factor_key = jnp.max(jnp.abs(latest_key), axis=0)
    ready_key = (latest_key / factor_key).astype(jnp.bfloat16)
    factor_value = jnp.max(jnp.abs(latest_value), axis=0)
    ready_value = (latest_value / factor_value).astype(jnp.bfloat16)
    serve_norm = (norm_train + norm_step).astype(jnp.bfloat16)
    return ready_query, ready_key, ready_value, factor_query, factor_key, factor_value, serve_norm
```

```python
import functools

import jax
import jax.numpy as jnp
from jax import lax
from jax.experimental import pallas as pl
from jax.experimental.pallas import tpu as pltpu
from jax.sharding import PartitionSpec as P

MESH = pl.DeviceIdType.MESH
mix_rate = 2.0

Z = X = 4
TP = 8
ROWS = 768
COLS = 1536
MINE = 96
HALF = MINE // 2
GROUP = MINE * X
RANK = 64
WHOLE = 12288
STEPS = (1, 3, 2)
DIAGONAL = [(a, b) for a in STEPS for b in STEPS]


def rows_at(start, size):
    return pl.ds(pl.multiple_of(start, 16), size)


def lanes_at(start, size):
    return pl.ds(pl.multiple_of(start, 128), size)


def kernel(
    w0, l0, h0, w1, l1, h1, w2, l2, h2, train, step,
    o0, o1, o2, f0, f1, f2, norm,
    w, low, high, latest, turned, rel_z, rel_x, max_z, max_x, inverse, adds, gains,
    load_sem, max_send, max_recv, gain_send, gain_recv, send, recv, own_sem,
):
    me = lax.axis_index("fsdp")
    tp = lax.axis_index("tp")
    z, x = me // X, me % X
    outs, factors = (o0, o1, o2), (f0, f1, f2)

    def at(dz, dx):
        return ((z + dz) % Z) * X + (x + dx) % X

    def remote(src, dst, s, r, dz, dx):
        return pltpu.make_async_remote_copy(
            src, dst, s, r, device_id={"fsdp": at(dz, dx)}, device_id_type=MESH
        )

    loads = []
    for m, (a, b, c) in enumerate(((w0, l0, h0), (w1, l1, h1), (w2, l2, h2))):
        loads.append(
            [
                pltpu.make_async_copy(b, low.at[m], load_sem.at[3 * m + 1]),
                pltpu.make_async_copy(c, high.at[m], load_sem.at[3 * m + 2]),
                pltpu.make_async_copy(a, w.at[m], load_sem.at[3 * m]),
            ]
        )
    extra = [
        pltpu.make_async_copy(train, adds.at[0], load_sem.at[9]),
        pltpu.make_async_copy(step, adds.at[1], load_sem.at[10]),
    ]
    for c in (*loads[0], *extra, *loads[1], *loads[2]):
        c.start()

    barrier = pltpu.get_barrier_semaphore()
    for d in (1, 2, 3):
        for peer in (at(d, 0), at(0, d)):
            pl.semaphore_signal(barrier, 1, device_id={"fsdp": peer}, device_id_type=MESH)
    for d in range(1, TP):
        pl.semaphore_signal(
            barrier, 1, device_id={"tp": (tp + d) % TP}, device_id_type=MESH
        )

    eye = (
        lax.broadcasted_iota(jnp.int32, (128, 128), 0)
        == lax.broadcasted_iota(jnp.int32, (128, 128), 1)
    ).astype(jnp.bfloat16)

    def merge(m):
        for c in loads[m]:
            c.wait()

        def columns(i, _):
            cols = lanes_at(i * 256, 256)
            most = jnp.zeros((1, 256), jnp.float32)
            for r in range(0, ROWS, 256):
                product = lax.dot_general(
                    low[m, :, r : r + 256],
                    high[m, :, cols],
                    (((0,), (0,)), ((), ())),
                    preferred_element_type=jnp.float32,
                )
                sums = w[m, r : r + 256, cols].astype(jnp.float32) + mix_rate * product
                latest[m, r : r + 256, cols] = sums
                most = jnp.maximum(most, jnp.max(jnp.abs(sums), axis=0, keepdims=True))
            max_z[m, z, :, cols] = most
            return 0

        lax.fori_loop(0, COLS // 256, columns, 0)

    def max_copies(m, stage):
        buffer, place = ((max_z, z), (max_x, x))[stage]
        return [
            remote(
                buffer.at[m, place],
                buffer.at[m, place],
                max_send.at[m, stage, d - 1],
                max_recv.at[m, stage, d - 1],
                *((d, 0) if stage == 0 else (0, d)),
            )
            for d in STEPS
        ]

    def start(copies):
        for c in copies:
            c.start()
        return copies

    def largest(buffer, m):
        return jnp.maximum(
            jnp.maximum(buffer[m, 0], buffer[m, 1]), jnp.maximum(buffer[m, 2], buffer[m, 3])
        )

    def wait_recv(copies):
        for c in copies:
            c.wait_recv()

    def second_stage(m, first):
        wait_recv(first)
        max_x[m, x] = largest(max_z, m)
        return start(max_copies(m, 1))

    def finish_max(m, second):
        wait_recv(second)
        factor = largest(max_x, m)
        factors[m][...] = pltpu.roll(factor, (COLS - MINE * me) % COLS, 1)[:, :MINE]
        inverse[m] = 1.0 / factor

    def turn(m, dz):
        base = ((z + dz) % Z) * GROUP
        for j in range(0, GROUP, 128):
            cols = lanes_at(base + j, 128)
            ready = (latest[m, :, cols] * inverse[m, :, cols]).astype(jnp.bfloat16)
            turned[m, lanes_at(base + j, 128), :] = lax.dot_general(
                eye, ready, (((1,), (1,)), ((), ())), preferred_element_type=jnp.float32
            ).astype(jnp.bfloat16)

    def block(m, dz, dx, first, size):
        return turned.at[m, rows_at(at(dz, dx) * MINE + first, size), :]

    def place_of(m, first, size, dz, dx):
        return outs[m].at[first : first + size, lanes_at(at(dz, dx) * ROWS, ROWS)]

    def straight(m, dz, dx):
        n = dz - 1 if dz else 2 + dx
        return remote(
            block(m, dz, dx, 0, MINE),
            place_of(m, 0, MINE, 0, 0),
            send.at[m, n],
            recv.at[m, n],
            dz,
            dx,
        )

    def number(dz, dx):
        return 3 * (dz - 1) + dx - 1

    def first_z(m, dz, dx):
        n = 6 + number(dz, dx)
        return remote(
            block(m, dz, dx, 0, HALF),
            rel_z.at[m, dz - 1, dx - 1],
            send.at[m, n],
            recv.at[m, n],
            dz,
            0,
        )

    def first_x(m, dz, dx):
        n = 15 + number(dz, dx)
        return remote(
            block(m, dz, dx, HALF, HALF),
            rel_x.at[m, dz - 1, dx - 1],
            send.at[m, n],
            recv.at[m, n],
            0,
            dx,
        )

    def then_x(m, dz, dx):
        n = 24 + number(dz, dx)
        return remote(
            rel_z.at[m, dz - 1, dx - 1],
            place_of(m, 0, HALF, -dz, 0),
            send.at[m, n],
            recv.at[m, n],
            0,
            dx,
        )

    def then_z(m, dz, dx):
        n = 33 + number(dz, dx)
        return remote(
            rel_x.at[m, dz - 1, dx - 1],
            place_of(m, HALF, HALF, 0, -dx),
            send.at[m, n],
            recv.at[m, n],
            dz,
            0,
        )

    sent, landing = [], []

    def send_group(m):
        relayed = []
        for dz in (*STEPS, 0):
            turn(m, dz)
            if dz:
                direct = [straight(m, dz, 0)]
                hops = [c(m, dz, dx) for dx in STEPS for c in (first_x, first_z)]
            else:
                direct = [straight(m, 0, dx) for dx in STEPS]
                hops = []
            start(direct)
            start(hops)
            sent.extend(direct + hops)
            landing.extend(direct)
            relayed.extend(hops)
        own = pltpu.make_async_copy(
            block(m, 0, 0, 0, MINE), place_of(m, 0, MINE, 0, 0), own_sem.at[m]
        )
        own.start()
        owns.append(own)

    owns = []

    def relay(m):
        for dz, dx in DIAGONAL:
            first_x(m, dz, dx).wait_recv()
            a = then_z(m, dz, dx)
            a.start()
            first_z(m, dz, dx).wait_recv()
            b = then_x(m, dz, dx)
            b.start()
            sent.extend((a, b))
            landing.extend((a, b))

    merge(0)
    pl.semaphore_wait(barrier, 13)
    first = [start(max_copies(0, 0))]

    for c in extra:
        c.wait()
    gains[z, x, tp, :, 0:MINE] = adds[0] + adds[1]

    def gain_copy(part, n, **device):
        return pltpu.make_async_remote_copy(
            part, part, gain_send.at[n], gain_recv.at[n], device_id=device, device_id_type=MESH
        )

    gain_z = start([gain_copy(gains.at[z, x, tp], d - 1, fsdp=at(d, 0)) for d in STEPS])

    merge(1)
    second = [second_stage(0, first[0])]
    first.append(start(max_copies(1, 0)))
    merge(2)
    first.append(start(max_copies(2, 0)))
    finish_max(0, second[0])
    send_group(0)
    second.append(second_stage(1, first[1]))
    second.append(second_stage(2, first[2]))
    wait_recv(gain_z)
    gain_x = start([gain_copy(gains.at[:, x, tp], 2 + d, fsdp=at(0, d)) for d in STEPS])
    finish_max(1, second[1])
    send_group(1)
    finish_max(2, second[2])
    wait_recv(gain_x)
    gain_tp = start(
        [gain_copy(gains.at[:, :, tp], 5 + d, tp=(tp + d) % TP) for d in range(1, TP)]
    )
    relay(0)
    send_group(2)
    relay(1)
    relay(2)
    wait_recv(gain_tp)
    norm[...] = gains[...]
    wait_recv(landing)
    for c in owns:
        c.wait()
    for c in (*sum(first, []), *sum(second, []), *gain_z, *gain_x, *gain_tp, *sent):
        c.wait_send()


def local(w0, l0, h0, w1, l1, h1, w2, l2, h2, train, step):
    f32, bf16 = jnp.float32, jnp.bfloat16
    vmem = pl.BlockSpec(memory_space=pltpu.VMEM)
    dma = pltpu.SemaphoreType.DMA
    o0, o1, o2, f0, f1, f2, norm = pl.pallas_call(
        kernel,
        out_shape=[
            *[pltpu.VMEM((MINE, WHOLE), bf16)] * 3,
            *[pltpu.VMEM((1, MINE), f32)] * 3,
            pltpu.VMEM((Z, X, TP, 1, 128), f32),
        ],
        in_specs=[pl.BlockSpec(memory_space=pltpu.HBM)] * 11,
        out_specs=[vmem] * 7,
        scratch_shapes=[
            pltpu.VMEM((3, ROWS, COLS), bf16),
            pltpu.VMEM((3, RANK, ROWS), bf16),
            pltpu.VMEM((3, RANK, COLS), bf16),
            pltpu.VMEM((3, ROWS, COLS), f32),
            pltpu.VMEM((3, COLS, ROWS), bf16),
            pltpu.VMEM((3, 3, 3, HALF, ROWS), bf16),
            pltpu.VMEM((3, 3, 3, HALF, ROWS), bf16),
            pltpu.VMEM((3, Z, 1, COLS), f32),
            pltpu.VMEM((3, X, 1, COLS), f32),
            pltpu.VMEM((3, 1, COLS), f32),
            pltpu.VMEM((2, 1, MINE), f32),
            pltpu.VMEM((Z, X, TP, 1, 128), f32),
            dma((11,)),
            dma((3, 2, 3)),
            dma((3, 2, 3)),
            dma((13,)),
            dma((13,)),
            dma((3, 42)),
            dma((3, 42)),
            dma((3,)),
        ],
        compiler_params=pltpu.CompilerParams(
            collective_id=0, has_side_effects=True, vmem_limit_bytes=42 * 1024 * 1024
        ),
        name="merge_and_spread",
    )(
        w0, l0.T, h0, w1, l1.T, h1, w2, l2.T, h2,
        train.reshape(1, MINE), step.reshape(1, MINE),
    )
    serve = norm.reshape(Z * X * TP, 128)[:, :MINE].reshape(WHOLE).astype(bf16)
    return (
        o0.T, o1.T, o2.T,
        f0.reshape(MINE), f1.reshape(MINE), f2.reshape(MINE),
        serve,
    )


def solution(mesh):
    return jax.shard_map(
        local,
        mesh=mesh,
        in_specs=(
            *(P("fsdp", "tp"), P("fsdp", None), P(None, "tp")) * 3,
            P(("fsdp", "tp")),
            P(("fsdp", "tp")),
        ),
        out_specs=(*[P(None, ("tp", "fsdp"))] * 3, *[P(("tp", "fsdp"))] * 3, P()),
        check_vma=False,
    )
```

```python
import functools

import jax
import jax.numpy as jnp
from jax import lax
from jax.experimental import pallas as pl
from jax.experimental.pallas import tpu as pltpu
from jax.sharding import PartitionSpec as P

MESH = pl.DeviceIdType.MESH
mix_rate = 2.0

Z = X = 4
TP = 8
ROWS = 768
COLS = 1536
MINE = 96
HALF = MINE // 2
GROUP = MINE * X
RANK = 64
WHOLE = 12288
PIECE = ROWS // 2
VMEM = 59_800_000
STEPS = (1, 3, 2)
ROUNDS = [(STEPS[i], STEPS[(i + r) % 3]) for r in range(3) for i in range(3)]


def rows_at(start, size):
    return pl.ds(pl.multiple_of(start, 16), size)


def lanes_at(start, size):
    return pl.ds(pl.multiple_of(start, 128), size)


def kernel(
    w0, l0, h0, w1, l1, h1, w2, l2, h2, train, step,
    o0, o1, o2, f0, f1, f2, norm,
    w, low, high, latest, sums0, turned, rel_z, rel_x, max_z, max_x, inverse, adds, gains, dense, lows,
    load_sem, max_send, max_recv, gain_send, gain_recv, low_send, low_recv, send, recv, own_sem, entered,
):
    me = lax.axis_index("fsdp")
    tp = lax.axis_index("tp")
    z, x = me // X, me % X
    outs, factors = (o0, o1, o2), (f0, f1, f2)

    def at(dz, dx):
        return ((z + dz) % Z) * X + (x + dx) % X

    def remote(src, dst, s, r, dz, dx):
        return pltpu.make_async_remote_copy(
            src, dst, s, r, device_id={"fsdp": at(dz, dx)}, device_id_type=MESH
        )

    y, core = tp // 2, tp % 2
    own_low = lows.at[core, rows_at(16 * y, 16), lanes_at((X * x + z) * PIECE, PIECE)]
    first_loads = [
        pltpu.make_async_copy(
            w0.at[:, j * GROUP : (j + 1) * GROUP],
            w.at[0, :, j * GROUP : (j + 1) * GROUP],
            load_sem.at[j],
        )
        for j in range(Z)
    ]
    loads = [
        [
            pltpu.make_async_copy(a, low.at[m], load_sem.at[4 + 3 * m]),
            pltpu.make_async_copy(b, high.at[m], load_sem.at[5 + 3 * m]),
            pltpu.make_async_copy(c, w.at[1 + m], load_sem.at[6 + 3 * m]),
        ]
        for m, (a, b, c) in enumerate(((l1, h1, w1), (l2, h2, w2)))
    ]
    extra = [
        pltpu.make_async_copy(train, adds.at[0], load_sem.at[10]),
        pltpu.make_async_copy(step, adds.at[1], load_sem.at[11]),
        pltpu.make_async_copy(
            l0.at[rows_at(16 * y, 16), lanes_at(core * PIECE, PIECE)], own_low, load_sem.at[12]
        ),
        pltpu.make_async_copy(h0, high.at[2], load_sem.at[13]),
    ]
    for c in (*first_loads, *loads[0], *loads[1], *extra):
        c.start()

    barrier = pltpu.get_barrier_semaphore()
    for d in (1, 2, 3):
        for peer in (at(d, 0), at(0, d)):
            pl.semaphore_signal(barrier, 1, device_id={"fsdp": peer}, device_id_type=MESH)
    for d in range(1, TP):

        @pl.when(tp + d < TP)
        def _():
            pl.semaphore_signal(
                barrier, 1, device_id={"tp": (tp + d) % TP}, device_id_type=MESH
            )

    eye = (
        lax.broadcasted_iota(jnp.int32, (128, 128), 0)
        == lax.broadcasted_iota(jnp.int32, (128, 128), 1)
    ).astype(jnp.bfloat16)

    def merge(m):
        for c in loads[m]:
            c.wait()

        def columns(i, _):
            cols = lanes_at(i * 256, 256)
            most = jnp.zeros((1, 256), jnp.float32)
            for r in range(0, ROWS, 256):
                product = lax.dot_general(
                    low[m, :, r : r + 256],
                    high[m, :, cols],
                    (((0,), (0,)), ((), ())),
                    preferred_element_type=jnp.float32,
                )
                sums = w[1 + m, r : r + 256, cols].astype(jnp.float32) + mix_rate * product
                latest[m, r : r + 256, cols] = sums
                most = jnp.maximum(most, jnp.max(jnp.abs(sums), axis=0, keepdims=True))
            max_z[z, m, :, cols] = most
            return 0

        lax.fori_loop(0, COLS // 256, columns, 0)

    def max_copies(stage):
        buffer, place = ((max_z, z), (max_x, x))[stage]
        return [
            remote(
                buffer.at[place],
                buffer.at[place],
                max_send.at[stage, d - 1],
                max_recv.at[stage, d - 1],
                *((d, 0) if stage == 0 else (0, d)),
            )
            for d in STEPS
        ]

    def start(copies):
        for c in copies:
            c.start()
        return copies

    def largest(buffer):
        return jnp.maximum(
            jnp.maximum(buffer[0], buffer[1]), jnp.maximum(buffer[2], buffer[3])
        )

    def wait_recv(copies):
        for c in copies:
            c.wait_recv()

    def transposed(block):
        return lax.dot_general(
            eye, block, (((1,), (1,)), ((), ())), preferred_element_type=jnp.float32
        ).astype(jnp.bfloat16)

    def turn(m):
        def columns(i, _):
            cols = lanes_at(i * 128, 128)
            ready = latest[m, :, cols] * inverse[m, :, cols]
            turned[1 + m, cols, :] = transposed(ready.astype(jnp.bfloat16))
            return 0

        lax.fori_loop(0, COLS // 128, columns, 0)

    def turn_first():
        for j, c in enumerate(first_loads):
            c.wait()
            for i in range(j * GROUP, (j + 1) * GROUP, 128):
                turned[0, i : i + 128, :] = transposed(w[0, :, i : i + 128])

    def finish_first():
        mine = pltpu.roll(high[2].astype(jnp.float32), (COLS - MINE * me) % COLS, 1)
        mine = mine[:, :MINE].astype(jnp.bfloat16)

        def place(i):
            p, c = i // 2, i % 2
            at_source = ((p % Z) * X + p // Z) * ROWS + c * PIECE
            return c, lanes_at(p * PIECE, PIECE), lanes_at(at_source, PIECE)

        def add(i, most):
            c, there, here = place(i)
            product = lax.dot_general(
                mine,
                lows[c, :, there],
                (((0,), (0,)), ((), ())),
                preferred_element_type=jnp.float32,
            )
            sums = o0[:, here].astype(jnp.float32) + mix_rate * product
            sums0[:, here] = sums
            sums = jnp.abs(sums)
            for j in range(0, PIECE, 128):
                most = jnp.maximum(most, sums[:, j : j + 128])
            return most

        most = lax.fori_loop(0, 2 * Z * X, add, jnp.zeros((MINE, 128), jnp.float32))
        factor = jnp.max(most, axis=1, keepdims=True)
        same = lax.broadcasted_iota(jnp.int32, (MINE, MINE), 0) == lax.broadcasted_iota(
            jnp.int32, (MINE, MINE), 1
        )
        f0[...] = jnp.max(jnp.where(same, factor, 0.0), axis=0, keepdims=True)
        scale = 1.0 / factor

        def divide(i, _):
            here = lanes_at(i * PIECE, PIECE)
            o0[:, here] = (sums0[:, here] * scale).astype(jnp.bfloat16)
            return 0

        lax.fori_loop(0, 2 * Z * X, divide, 0)

    def block(m, dz, dx, first, size):
        return turned.at[m, rows_at(at(dz, dx) * MINE + first, size), :]

    def place_of(m, first, size, dz, dx):
        return outs[m].at[first : first + size, lanes_at(at(dz, dx) * ROWS, ROWS)]

    def straight(m, dz, dx):
        n = dz - 1 if dz else 2 + dx
        return remote(
            block(m, dz, dx, 0, MINE),
            place_of(m, 0, MINE, 0, 0),
            send.at[m, n],
            recv.at[m, n],
            dz,
            dx,
        )

    def number(dz, dx):
        return 3 * (dz - 1) + dx - 1

    def first_z(m, dz, dx):
        n = 6 + number(dz, dx)
        return remote(
            block(m, dz, dx, 0, HALF),
            rel_z.at[m, dz - 1, dx - 1],
            send.at[m, n],
            recv.at[m, n],
            dz,
            0,
        )

    def first_x(m, dz, dx):
        n = 15 + number(dz, dx)
        return remote(
            block(m, dz, dx, HALF, HALF),
            rel_x.at[m, dz - 1, dx - 1],
            send.at[m, n],
            recv.at[m, n],
            0,
            dx,
        )

    def then_x(m, dz, dx):
        n = 24 + number(dz, dx)
        return remote(
            rel_z.at[m, dz - 1, dx - 1],
            place_of(m, 0, HALF, -dz, 0),
            send.at[m, n],
            recv.at[m, n],
            0,
            dx,
        )

    def then_z(m, dz, dx):
        n = 33 + number(dz, dx)
        return remote(
            rel_x.at[m, dz - 1, dx - 1],
            place_of(m, HALF, HALF, 0, -dx),
            send.at[m, n],
            recv.at[m, n],
            dz,
            0,
        )

    sent, landing, owns = [], [[], [], []], []

    def send_hops(m):
        sent.extend(
            start(
                [c(m, *d) for a, b in ROUNDS for c, d in ((first_z, (a, b)), (first_x, (b, a)))]
            )
        )

    def send_straight(m):
        copies = start([straight(m, *d) for a in STEPS for d in ((a, 0), (0, a))])
        sent.extend(copies)
        landing[m].extend(copies)
        own = pltpu.make_async_copy(
            block(m, 0, 0, 0, MINE), place_of(m, 0, MINE, 0, 0), own_sem.at[m]
        )
        own.start()
        owns.append(own)

    def relay(m):
        for a, b in ROUNDS:
            first_x(m, a, b).wait_recv()
            first_z(m, b, a).wait_recv()
            sent.extend(start([then_z(m, a, b), then_x(m, b, a)]))
            landing[m].extend(sent[-2:])

    turn_first()
    pl.semaphore_wait(barrier, 6 + tp)
    send_hops(0)
    for d in range(1, TP):

        @pl.when(d <= tp)
        def _():
            pl.semaphore_signal(
                entered, 1, device_id={"tp": (tp + TP - d) % TP}, device_id_type=MESH
            )

    def share(part, s, r, n, **device):
        return pltpu.make_async_remote_copy(
            part, part, s.at[n], r.at[n], device_id=device, device_id_type=MESH
        )

    def gather(stage):
        if stage == 0:
            parts = gains.at[z, x, tp], own_low
            targets = [(d - 1, {"fsdp": at(d, 0)}) for d in STEPS]
        elif stage == 1:
            lanes = lanes_at(X * x * PIECE, Z * PIECE)
            parts = gains.at[:, x, tp], lows.at[core, rows_at(16 * y, 16), lanes]
            targets = [(2 + d, {"fsdp": at(0, d)}) for d in STEPS]
        else:
            parts = gains.at[:, :, tp], lows.at[core, rows_at(16 * y, 16), :]
            targets = [(5 + d, {"tp": (tp + d) % TP}) for d in range(1, TP)]
        sems = (gain_send, gain_recv), (low_send, low_recv)
        return start([share(p, *q, n, **t) for n, t in targets for p, q in zip(parts, sems)])

    merge(0)
    merge(1)
    small = [start(max_copies(0))]
    for c in extra:
        c.wait()
    gains[z, x, tp, :, 0:MINE] = adds[0] + adds[1]
    small.append(gather(0))
    send_straight(0)
    wait_recv(small[0])
    max_x[x] = largest(max_z)
    small.append(start(max_copies(1)))
    wait_recv(small[1])
    small.append(gather(1))
    relay(0)
    wait_recv(small[2])
    factor = largest(max_x)
    inverse[...] = 1.0 / factor
    for m in (0, 1):
        outputs = pltpu.roll(factor[m], (COLS - MINE * me) % COLS, 1)
        factors[1 + m][...] = outputs[:, :MINE]
    turn(0)
    send_hops(1)
    send_straight(1)
    wait_recv(small[3])

    @pl.when(tp < TP - 1)
    def _():
        pl.semaphore_wait(entered, TP - 1 - tp)

    small.append(gather(2))
    turn(1)
    send_hops(2)
    send_straight(2)
    wait_recv(landing[0])
    owns[0].wait()
    wait_recv(small[4])
    finish_first()
    relay(1)
    relay(2)
    lane = lax.broadcasted_iota(jnp.int32, (1, 128), 1)

    def pack(g, _):
        f, t = g // 2, 4 * (g % 2)
        a, b, c, d = (gains[f // X, f % X, t + j] for j in range(4))
        b, c, d = pltpu.roll(b, 96, 1), pltpu.roll(c, 64, 1), pltpu.roll(d, 32, 1)
        dense[pl.ds(3 * g, 1), :] = jnp.where(lane < 96, a, b)
        dense[pl.ds(3 * g + 1, 1), :] = jnp.where(lane < 64, b, c)
        dense[pl.ds(3 * g + 2, 1), :] = jnp.where(lane < 32, c, d)
        return 0

    lax.fori_loop(0, Z * X * TP // 4, pack, 0)
    norm[...] = dense[...].astype(jnp.bfloat16)
    wait_recv(landing[1] + landing[2])
    for c in owns[1:]:
        c.wait()
    for c in (*sum(small, []), *sent):
        c.wait_send()


def write_out(*refs):
    copies = [
        pltpu.make_async_copy(a, b, refs[14].at[n])
        for n, (a, b) in enumerate(zip(refs[:7], refs[7:14]))
    ]
    for c in copies:
        c.start()
    for c in copies:
        c.wait()


def local(w0, l0, h0, w1, l1, h1, w2, l2, h2, train, step):
    f32, bf16 = jnp.float32, jnp.bfloat16
    vmem = pl.BlockSpec(memory_space=pltpu.VMEM)
    dma = pltpu.SemaphoreType.DMA
    gathered = pl.pallas_call(
        kernel,
        out_shape=[
            *[pltpu.VMEM((MINE, WHOLE), bf16)] * 3,
            *[pltpu.VMEM((1, MINE), f32)] * 3,
            pltpu.VMEM((WHOLE // 128, 128), bf16),
        ],
        in_specs=[pl.BlockSpec(memory_space=pltpu.HBM)] * 11,
        out_specs=[vmem] * 7,
        scratch_shapes=[
            pltpu.VMEM((3, ROWS, COLS), bf16),
            pltpu.VMEM((2, RANK, ROWS), bf16),
            pltpu.VMEM((3, RANK, COLS), bf16),
            pltpu.VMEM((2, ROWS, COLS), f32),
            pltpu.VMEM((MINE, WHOLE), f32),
            pltpu.VMEM((3, COLS, ROWS), bf16),
            pltpu.VMEM((3, 3, 3, HALF, ROWS), bf16),
            pltpu.VMEM((3, 3, 3, HALF, ROWS), bf16),
            pltpu.VMEM((Z, 2, 1, COLS), f32),
            pltpu.VMEM((X, 2, 1, COLS), f32),
            pltpu.VMEM((2, 1, COLS), f32),
            pltpu.VMEM((2, 1, MINE), f32),
            pltpu.VMEM((Z, X, TP, 1, 128), f32),
            pltpu.VMEM((MINE, 128), f32),
            pltpu.VMEM((2, RANK, Z * X * PIECE), bf16),
            dma((14,)),
            dma((2, 3)),
            dma((2, 3)),
            dma((13,)),
            dma((13,)),
            dma((13,)),
            dma((13,)),
            dma((3, 42)),
            dma((3, 42)),
            dma((3,)),
            pltpu.SemaphoreType.REGULAR,
        ],
        compiler_params=pltpu.CompilerParams(
            collective_id=0, has_side_effects=True, vmem_limit_bytes=VMEM
        ),
        name="merge_and_spread",
    )(
        w0, l0.T, h0, w1, l1.T, h1, w2, l2.T, h2,
        train.reshape(1, MINE), step.reshape(1, MINE),
    )
    o0, o1, o2, f0, f1, f2, norm = pl.pallas_call(
        write_out,
        out_shape=[jax.ShapeDtypeStruct(a.shape, a.dtype) for a in gathered],
        in_specs=[pl.BlockSpec(memory_space=pl.ANY)] * 7,
        out_specs=[pl.BlockSpec(memory_space=pltpu.HBM)] * 7,
        scratch_shapes=[dma((7,))],
        compiler_params=pltpu.CompilerParams(vmem_limit_bytes=1024 * 1024),
        name="write_out",
    )(*gathered)
    return (
        o0.T, o1.T, o2.T,
        f0.reshape(MINE), f1.reshape(MINE), f2.reshape(MINE),
        norm.reshape(WHOLE),
    )


def solution(mesh):
    return jax.shard_map(
        local,
        mesh=mesh,
        in_specs=(
            *(P("fsdp", "tp"), P("fsdp", None), P(None, "tp")) * 3,
            P(("fsdp", "tp")),
            P(("fsdp", "tp")),
        ),
        out_specs=(*[P(None, ("tp", "fsdp"))] * 3, *[P(("tp", "fsdp"))] * 3, P()),
        check_vma=False,
    )
```

```python
import functools

import jax
import jax.numpy as jnp
from jax import lax
from jax.experimental import pallas as pl
from jax.experimental.pallas import tpu as pltpu
from jax.sharding import PartitionSpec as P

MESH = pl.DeviceIdType.MESH
mix_rate = 2.0

Z = X = 4
TP = 8
ROWS = 768
COLS = 1536
MINE = 96
HALF = MINE // 2
GROUP = MINE * X
RANK = 64
WHOLE = 12288
PIECE = ROWS // 2
VMEM = 59_800_000
STEPS = (1, 3, 2)
ROUNDS = [(STEPS[i], STEPS[(i + r) % 3]) for r in range(3) for i in range(3)]
LAST = sorted(ROUNDS, key=lambda d: d[0] != 2)


def rows_at(start, size):
    return pl.ds(pl.multiple_of(start, 16), size)


def lanes_at(start, size):
    return pl.ds(pl.multiple_of(start, 128), size)


def kernel(
    w0, l0, h0, w1, l1, h1, w2, l2, h2, train, step,
    o0, o1, o2, f0, f1, f2, norm,
    w, low, high, latest, sums0, turned, rel_z, rel_x, max_z, max_x, inverse, adds, gains, dense, lows,
    load_sem, max_send, max_recv, gain_send, gain_recv, low_send, low_recv, send, recv, own_sem, entered,
):
    me = lax.axis_index("fsdp")
    tp = lax.axis_index("tp")
    z, x = me // X, me % X
    outs, factors = (o0, o1, o2), (f0, f1, f2)

    def at(dz, dx):
        return ((z + dz) % Z) * X + (x + dx) % X

    def remote(src, dst, s, r, dz, dx):
        return pltpu.make_async_remote_copy(
            src, dst, s, r, device_id={"fsdp": at(dz, dx)}, device_id_type=MESH
        )

    y, core = tp // 2, tp % 2
    major, minor = x + core * (z - x), z + core * (x - z)
    own_low = lows.at[core, rows_at(16 * y, 16), lanes_at((X * major + minor) * PIECE, PIECE)]
    first_loads = [
        pltpu.make_async_copy(
            w0.at[:, j * GROUP : (j + 1) * GROUP],
            w.at[0, :, j * GROUP : (j + 1) * GROUP],
            load_sem.at[j],
        )
        for j in range(Z)
    ]
    loads = [
        [
            pltpu.make_async_copy(a, low.at[m], load_sem.at[4 + 3 * m]),
            pltpu.make_async_copy(b, high.at[m], load_sem.at[5 + 3 * m]),
            pltpu.make_async_copy(c, w.at[1 + m], load_sem.at[6 + 3 * m]),
        ]
        for m, (a, b, c) in enumerate(((l1, h1, w1), (l2, h2, w2)))
    ]
    extra = [
        pltpu.make_async_copy(train, adds.at[0], load_sem.at[10]),
        pltpu.make_async_copy(step, adds.at[1], load_sem.at[11]),
        pltpu.make_async_copy(
            l0.at[rows_at(16 * y, 16), lanes_at(core * PIECE, PIECE)], own_low, load_sem.at[12]
        ),
        pltpu.make_async_copy(h0, high.at[2], load_sem.at[13]),
    ]
    barrier = pltpu.get_barrier_semaphore()
    for d in (1, 2, 3):
        for peer in (at(d, 0), at(0, d)):
            pl.semaphore_signal(barrier, 1, device_id={"fsdp": peer}, device_id_type=MESH)
    for d in range(1, TP):

        @pl.when(tp + d < TP)
        def _():
            pl.semaphore_signal(
                barrier, 1, device_id={"tp": (tp + d) % TP}, device_id_type=MESH
            )

    for c in (*first_loads, *loads[0], *loads[1], *extra):
        c.start()

    eye = (
        lax.broadcasted_iota(jnp.int32, (128, 128), 0)
        == lax.broadcasted_iota(jnp.int32, (128, 128), 1)
    ).astype(jnp.bfloat16)

    def merge(m):
        for c in loads[m]:
            c.wait()

        def columns(i, _):
            cols = lanes_at(i * 256, 256)
            most = jnp.zeros((1, 256), jnp.float32)
            for r in range(0, ROWS, 256):
                product = lax.dot_general(
                    low[m, :, r : r + 256],
                    high[m, :, cols],
                    (((0,), (0,)), ((), ())),
                    preferred_element_type=jnp.float32,
                )
                sums = w[1 + m, r : r + 256, cols].astype(jnp.float32) + mix_rate * product
                latest[m, r : r + 256, cols] = sums
                most = jnp.maximum(most, jnp.max(jnp.abs(sums), axis=0, keepdims=True))
            max_z[z, m, :, cols] = most
            return 0

        lax.fori_loop(0, COLS // 256, columns, 0)

    def max_copies(stage):
        buffer, place = ((max_z, z), (max_x, x))[stage]
        return [
            remote(
                buffer.at[place],
                buffer.at[place],
                max_send.at[stage, d - 1],
                max_recv.at[stage, d - 1],
                *((d, 0) if stage == 0 else (0, d)),
            )
            for d in STEPS
        ]

    def start(copies):
        for c in copies:
            c.start()
        return copies

    def largest(buffer):
        return jnp.maximum(
            jnp.maximum(buffer[0], buffer[1]), jnp.maximum(buffer[2], buffer[3])
        )

    def wait_recv(copies):
        for c in copies:
            c.wait_recv()

    def transposed(block):
        return lax.dot_general(
            eye, block, (((1,), (1,)), ((), ())), preferred_element_type=jnp.float32
        ).astype(jnp.bfloat16)

    def turn(m):
        def columns(i, _):
            cols = lanes_at(i * 128, 128)
            ready = latest[m, :, cols] * inverse[m, :, cols]
            turned[1 + m, cols, :] = transposed(ready.astype(jnp.bfloat16))
            return 0

        lax.fori_loop(0, COLS // 128, columns, 0)

    def turn_first():
        for j, c in enumerate(first_loads):
            c.wait()
            for i in range(j * GROUP, (j + 1) * GROUP, 128):
                turned[0, i : i + 128, :] = transposed(w[0, :, i : i + 128])

    def finish_first():
        mine = pltpu.roll(high[2].astype(jnp.float32), (COLS - MINE * me) % COLS, 1)
        mine = mine[:, :MINE].astype(jnp.bfloat16)

        def place(i):
            p, c = i // 2, i % 2
            a, b = p // X, p % X
            at_source = ((b + c * (a - b)) * X + a + c * (b - a)) * ROWS + c * PIECE
            return c, lanes_at(p * PIECE, PIECE), lanes_at(at_source, PIECE)

        def add(i, most):
            c, there, here = place(i)
            product = lax.dot_general(
                mine,
                lows[c, :, there],
                (((0,), (0,)), ((), ())),
                preferred_element_type=jnp.float32,
            )
            sums = o0[:, here].astype(jnp.float32) + mix_rate * product
            sums0[:, here] = sums
            sums = jnp.abs(sums)
            for j in range(0, PIECE, 128):
                most = jnp.maximum(most, sums[:, j : j + 128])
            return most

        most = lax.fori_loop(0, 2 * Z * X, add, jnp.zeros((MINE, 128), jnp.float32))
        factor = jnp.max(most, axis=1, keepdims=True)
        same = lax.broadcasted_iota(jnp.int32, (MINE, MINE), 0) == lax.broadcasted_iota(
            jnp.int32, (MINE, MINE), 1
        )
        f0[...] = jnp.max(jnp.where(same, factor, 0.0), axis=0, keepdims=True)
        scale = 1.0 / factor

        def divide(i, _):
            here = lanes_at(i * PIECE, PIECE)
            o0[:, here] = (sums0[:, here] * scale).astype(jnp.bfloat16)
            return 0

        lax.fori_loop(0, 2 * Z * X, divide, 0)

    def block(m, dz, dx, first, size):
        return turned.at[m, rows_at(at(dz, dx) * MINE + first, size), :]

    def place_of(m, first, size, dz, dx):
        return outs[m].at[first : first + size, lanes_at(at(dz, dx) * ROWS, ROWS)]

    def straight(m, dz, dx):
        n = dz - 1 if dz else 2 + dx
        return remote(
            block(m, dz, dx, 0, MINE),
            place_of(m, 0, MINE, 0, 0),
            send.at[m, n],
            recv.at[m, n],
            dz,
            dx,
        )

    def number(dz, dx):
        return 3 * (dz - 1) + dx - 1

    def first_z(m, dz, dx):
        n = 6 + number(dz, dx)
        return remote(
            block(m, dz, dx, 0, HALF),
            rel_z.at[m, dz - 1, dx - 1],
            send.at[m, n],
            recv.at[m, n],
            dz,
            0,
        )

    def first_x(m, dz, dx):
        n = 15 + number(dz, dx)
        return remote(
            block(m, dz, dx, HALF, HALF),
            rel_x.at[m, dz - 1, dx - 1],
            send.at[m, n],
            recv.at[m, n],
            0,
            dx,
        )

    def then_x(m, dz, dx):
        n = 24 + number(dz, dx)
        return remote(
            rel_z.at[m, dz - 1, dx - 1],
            place_of(m, 0, HALF, -dz, 0),
            send.at[m, n],
            recv.at[m, n],
            0,
            dx,
        )

    def then_z(m, dz, dx):
        n = 33 + number(dz, dx)
        return remote(
            rel_x.at[m, dz - 1, dx - 1],
            place_of(m, HALF, HALF, 0, -dx),
            send.at[m, n],
            recv.at[m, n],
            dz,
            0,
        )

    sent, landing, owns = [], [[], [], []], []

    def hops_of(m):
        return [c(m, *d) for a, b in ROUNDS for c, d in ((first_z, (a, b)), (first_x, (b, a)))]

    def send_hops(m):
        sent.extend(start(hops_of(m)))

    def send_straight(m):
        copies = start([straight(m, *d) for a in STEPS for d in ((a, 0), (0, a))])
        sent.extend(copies)
        landing[m].extend(copies)
        own = pltpu.make_async_copy(
            block(m, 0, 0, 0, MINE), place_of(m, 0, MINE, 0, 0), own_sem.at[m]
        )
        own.start()
        owns.append(own)

    def relay(m):
        for a, b in (ROUNDS if m < 2 else LAST):
            first_x(m, a, b).wait_recv()
            first_z(m, b, a).wait_recv()
            sent.extend(start([then_z(m, a, b), then_x(m, b, a)]))
            landing[m].extend(sent[-2:])

    turn_first()
    pl.semaphore_wait(barrier, 6 + tp)
    at_first = hops_of(0)
    sent.extend(at_first)

    @pl.when(core == 1)
    def _():
        start(at_first)

    for d in range(1, TP):

        @pl.when(d <= tp)
        def _():
            pl.semaphore_signal(
                entered, 1, device_id={"tp": (tp + TP - d) % TP}, device_id_type=MESH
            )

    def share(part, s, r, n, **device):
        return pltpu.make_async_remote_copy(
            part, part, s.at[n], r.at[n], device_id=device, device_id_type=MESH
        )

    def gather(stage):
        if stage == 0:
            parts = gains.at[core, major, minor, y], own_low
            targets = [(d - 1, {"fsdp": at(d - core * d, core * d)}) for d in STEPS]
        elif stage == 1:
            lanes = lanes_at(X * major * PIECE, X * PIECE)
            parts = gains.at[core, major, :, y], lows.at[core, rows_at(16 * y, 16), lanes]
            targets = [(2 + d, {"fsdp": at(core * d, d - core * d)}) for d in STEPS]
        else:
            parts = gains.at[core, :, :, y], lows.at[core, rows_at(16 * y, 16), :]
            targets = [(5 + d, {"tp": (tp + d) % TP}) for d in range(1, TP)]
        sems = (gain_send, gain_recv), (low_send, low_recv)
        return start([share(p, *q, n, **t) for n, t in targets for p, q in zip(parts, sems)])

    merge(0)

    @pl.when(core == 0)
    def _():
        start(at_first)

    merge(1)
    small = [start(max_copies(0))]
    for c in extra:
        c.wait()
    gains[core, major, minor, y, :, 0:MINE] = adds[0] + adds[1]
    small.append(gather(0))
    send_straight(0)
    wait_recv(small[0])
    max_x[x] = largest(max_z)
    small.append(start(max_copies(1)))
    wait_recv(small[1])
    small.append(gather(1))
    relay(0)
    wait_recv(small[2])
    factor = largest(max_x)
    inverse[...] = 1.0 / factor
    for m in (0, 1):
        outputs = pltpu.roll(factor[m], (COLS - MINE * me) % COLS, 1)
        factors[1 + m][...] = outputs[:, :MINE]
    turn(0)
    send_hops(1)
    send_straight(1)
    wait_recv(small[3])

    @pl.when(tp < TP - 1)
    def _():
        pl.semaphore_wait(entered, TP - 1 - tp)

    small.append(gather(2))
    turn(1)
    send_hops(2)
    send_straight(2)
    wait_recv(landing[0])
    owns[0].wait()
    wait_recv(small[4])
    finish_first()
    relay(1)
    relay(2)
    lane = lax.broadcasted_iota(jnp.int32, (1, 128), 1)

    def pack(g, _):
        f = g // 2
        p, q, t = f // X, f % X, 2 * (g % 2)
        a, c = gains[0, q, p, t], gains[0, q, p, t + 1]
        b, d = gains[1, p, q, t], gains[1, p, q, t + 1]
        b, c, d = pltpu.roll(b, 96, 1), pltpu.roll(c, 64, 1), pltpu.roll(d, 32, 1)
        dense[pl.ds(3 * g, 1), :] = jnp.where(lane < 96, a, b)
        dense[pl.ds(3 * g + 1, 1), :] = jnp.where(lane < 64, b, c)
        dense[pl.ds(3 * g + 2, 1), :] = jnp.where(lane < 32, c, d)
        return 0

    lax.fori_loop(0, Z * X * TP // 4, pack, 0)
    norm[...] = dense[...].astype(jnp.bfloat16)
    for c in owns[1:]:
        c.wait()
    last = len(sent) - 2 * len(LAST)
    for c in (*sum(small, []), *sent[:last]):
        c.wait_send()
    wait_recv(landing[1] + landing[2])
    for c in sent[last:]:
        c.wait_send()


def write_out(*refs):
    copies = [
        pltpu.make_async_copy(a, b, refs[14].at[n])
        for n, (a, b) in enumerate(zip(refs[:7], refs[7:14]))
    ]
    for c in copies:
        c.start()
    for c in copies:
        c.wait()


def local(w0, l0, h0, w1, l1, h1, w2, l2, h2, train, step):
    f32, bf16 = jnp.float32, jnp.bfloat16
    vmem = pl.BlockSpec(memory_space=pltpu.VMEM)
    dma = pltpu.SemaphoreType.DMA
    gathered = pl.pallas_call(
        kernel,
        out_shape=[
            *[pltpu.VMEM((MINE, WHOLE), bf16)] * 3,
            *[pltpu.VMEM((1, MINE), f32)] * 3,
            pltpu.VMEM((WHOLE // 128, 128), bf16),
        ],
        in_specs=[pl.BlockSpec(memory_space=pltpu.HBM)] * 11,
        out_specs=[vmem] * 7,
        scratch_shapes=[
            pltpu.VMEM((3, ROWS, COLS), bf16),
            pltpu.VMEM((2, RANK, ROWS), bf16),
            pltpu.VMEM((3, RANK, COLS), bf16),
            pltpu.VMEM((2, ROWS, COLS), f32),
            pltpu.VMEM((MINE, WHOLE), f32),
            pltpu.VMEM((3, COLS, ROWS), bf16),
            pltpu.VMEM((3, 3, 3, HALF, ROWS), bf16),
            pltpu.VMEM((3, 3, 3, HALF, ROWS), bf16),
            pltpu.VMEM((Z, 2, 1, COLS), f32),
            pltpu.VMEM((X, 2, 1, COLS), f32),
            pltpu.VMEM((2, 1, COLS), f32),
            pltpu.VMEM((2, 1, MINE), f32),
            pltpu.VMEM((2, X, X, 4, 1, 128), f32),
            pltpu.VMEM((MINE, 128), f32),
            pltpu.VMEM((2, RANK, Z * X * PIECE), bf16),
            dma((14,)),
            dma((2, 3)),
            dma((2, 3)),
            dma((13,)),
            dma((13,)),
            dma((13,)),
            dma((13,)),
            dma((3, 42)),
            dma((3, 42)),
            dma((3,)),
            pltpu.SemaphoreType.REGULAR,
        ],
        compiler_params=pltpu.CompilerParams(
            collective_id=0, has_side_effects=True, vmem_limit_bytes=VMEM
        ),
        name="merge_and_spread",
    )(
        w0, l0.T, h0, w1, l1.T, h1, w2, l2.T, h2,
        train.reshape(1, MINE), step.reshape(1, MINE),
    )
    o0, o1, o2, f0, f1, f2, norm = pl.pallas_call(
        write_out,
        out_shape=[jax.ShapeDtypeStruct(a.shape, a.dtype) for a in gathered],
        in_specs=[pl.BlockSpec(memory_space=pl.ANY)] * 7,
        out_specs=[pl.BlockSpec(memory_space=pltpu.HBM)] * 7,
        scratch_shapes=[dma((7,))],
        compiler_params=pltpu.CompilerParams(vmem_limit_bytes=1024 * 1024),
        name="write_out",
    )(*gathered)
    return (
        o0.T, o1.T, o2.T,
        f0.reshape(MINE), f1.reshape(MINE), f2.reshape(MINE),
        norm.reshape(WHOLE),
    )


def solution(mesh):
    return jax.shard_map(
        local,
        mesh=mesh,
        in_specs=(
            *(P("fsdp", "tp"), P("fsdp", None), P(None, "tp")) * 3,
            P(("fsdp", "tp")),
            P(("fsdp", "tp")),
        ),
        out_specs=(*[P(None, ("tp", "fsdp"))] * 3, *[P(("tp", "fsdp"))] * 3, P()),
        check_vma=False,
    )
```

```python
import functools

import jax
import jax.numpy as jnp
from jax import lax
from jax.experimental import pallas as pl
from jax.experimental.pallas import tpu as pltpu
from jax.sharding import PartitionSpec as P

MESH = pl.DeviceIdType.MESH
mix_rate = 2.0

Z = X = 4
TP = 8
ROWS = 768
COLS = 1536
MINE = 96
HALF = MINE // 2
GROUP = MINE * X
RANK = 64
WHOLE = 12288
PIECE = ROWS // 2
VMEM = 59_800_000
STEPS = (1, 3, 2)
ROUNDS = [(STEPS[i], STEPS[(i + r) % 3]) for r in range(3) for i in range(3)]
LAST = sorted(ROUNDS, key=lambda d: d[0] != 2)


def rows_at(start, size):
    return pl.ds(pl.multiple_of(start, 16), size)


def lanes_at(start, size):
    return pl.ds(pl.multiple_of(start, 128), size)


def kernel(
    w0, l0, h0, w1, l1, h1, w2, l2, h2, train, step,
    o0, o1, o2, f0, f1, f2, norm,
    w, low, high, latest, sums0, turned, rel_z, rel_x, max_z, max_x, inverse, adds, gains, dense, lows,
    load_sem, max_send, max_recv, gain_send, gain_recv, low_send, low_recv, send, recv, own_sem, entered,
):
    me = lax.axis_index("fsdp")
    tp = lax.axis_index("tp")
    z, x = me // X, me % X
    y, core = tp // 2, tp % 2
    way = 2 * core - 1
    outs, factors = (o0, o1, o2), (f0, f1, f2)

    def at(dz, dx):
        return ((z + way * dz + Z) % Z) * X + (x + way * dx + X) % X

    def remote(src, dst, s, r, dz, dx):
        return pltpu.make_async_remote_copy(
            src, dst, s, r, device_id={"fsdp": at(dz, dx)}, device_id_type=MESH
        )

    major, minor = x + core * (z - x), z + core * (x - z)
    own_low = lows.at[core, rows_at(16 * y, 16), lanes_at((X * major + minor) * PIECE, PIECE)]
    first_loads = [
        pltpu.make_async_copy(
            w0.at[:, j * GROUP : (j + 1) * GROUP],
            w.at[0, :, j * GROUP : (j + 1) * GROUP],
            load_sem.at[j],
        )
        for j in range(Z)
    ]
    loads = [
        [
            pltpu.make_async_copy(a, low.at[m], load_sem.at[4 + 3 * m]),
            pltpu.make_async_copy(b, high.at[m], load_sem.at[5 + 3 * m]),
            pltpu.make_async_copy(c, w.at[1 + m], load_sem.at[6 + 3 * m]),
        ]
        for m, (a, b, c) in enumerate(((l1, h1, w1), (l2, h2, w2)))
    ]
    extra = [
        pltpu.make_async_copy(train, adds.at[0], load_sem.at[10]),
        pltpu.make_async_copy(step, adds.at[1], load_sem.at[11]),
        pltpu.make_async_copy(
            l0.at[rows_at(16 * y, 16), lanes_at(core * PIECE, PIECE)], own_low, load_sem.at[12]
        ),
        pltpu.make_async_copy(h0, high.at[2], load_sem.at[13]),
    ]
    barrier = pltpu.get_barrier_semaphore()
    for d in (1, 2, 3):
        for peer in (at(d, 0), at(0, d)):
            pl.semaphore_signal(barrier, 1, device_id={"fsdp": peer}, device_id_type=MESH)
    for d in range(1, TP):

        @pl.when(tp + d < TP)
        def _():
            pl.semaphore_signal(
                barrier, 1, device_id={"tp": (tp + d) % TP}, device_id_type=MESH
            )

    for c in (*first_loads, *loads[0], *loads[1], *extra):
        c.start()

    eye = (
        lax.broadcasted_iota(jnp.int32, (128, 128), 0)
        == lax.broadcasted_iota(jnp.int32, (128, 128), 1)
    ).astype(jnp.bfloat16)

    def merge(m):
        for c in loads[m]:
            c.wait()

        def columns(i, _):
            cols = lanes_at(i * 256, 256)
            most = jnp.zeros((1, 256), jnp.float32)
            for r in range(0, ROWS, 256):
                product = lax.dot_general(
                    low[m, :, r : r + 256],
                    high[m, :, cols],
                    (((0,), (0,)), ((), ())),
                    preferred_element_type=jnp.float32,
                )
                sums = w[1 + m, r : r + 256, cols].astype(jnp.float32) + mix_rate * product
                latest[m, r : r + 256, cols] = sums
                most = jnp.maximum(most, jnp.max(jnp.abs(sums), axis=0, keepdims=True))
            max_z[z, m, :, cols] = most
            return 0

        lax.fori_loop(0, COLS // 256, columns, 0)

    def max_copies(stage):
        buffer, place = ((max_z, z), (max_x, x))[stage]
        return [
            remote(
                buffer.at[place],
                buffer.at[place],
                max_send.at[stage, d - 1],
                max_recv.at[stage, d - 1],
                *((d, 0) if stage == 0 else (0, d)),
            )
            for d in STEPS
        ]

    def start(copies):
        for c in copies:
            c.start()
        return copies

    def largest(buffer):
        return jnp.maximum(
            jnp.maximum(buffer[0], buffer[1]), jnp.maximum(buffer[2], buffer[3])
        )

    def wait_recv(copies):
        for c in copies:
            c.wait_recv()

    def transposed(block):
        return lax.dot_general(
            eye, block, (((1,), (1,)), ((), ())), preferred_element_type=jnp.float32
        ).astype(jnp.bfloat16)

    def turn(m):
        def columns(i, _):
            cols = lanes_at(i * 128, 128)
            ready = latest[m, :, cols] * inverse[m, :, cols]
            turned[1 + m, cols, :] = transposed(ready.astype(jnp.bfloat16))
            return 0

        lax.fori_loop(0, COLS // 128, columns, 0)

    def turn_first():
        for j, c in enumerate(first_loads):
            c.wait()
            for i in range(j * GROUP, (j + 1) * GROUP, 128):
                turned[0, i : i + 128, :] = transposed(w[0, :, i : i + 128])

    def finish_first():
        mine = pltpu.roll(high[2].astype(jnp.float32), (COLS - MINE * me) % COLS, 1)
        mine = mine[:, :MINE].astype(jnp.bfloat16)

        def place(i):
            p, c = i // 2, i % 2
            a, b = p // X, p % X
            at_source = ((b + c * (a - b)) * X + a + c * (b - a)) * ROWS + c * PIECE
            return c, lanes_at(p * PIECE, PIECE), lanes_at(at_source, PIECE)

        def add(i, most):
            c, there, here = place(i)
            product = lax.dot_general(
                mine,
                lows[c, :, there],
                (((0,), (0,)), ((), ())),
                preferred_element_type=jnp.float32,
            )
            sums = o0[:, here].astype(jnp.float32) + mix_rate * product
            sums0[:, here] = sums
            sums = jnp.abs(sums)
            for j in range(0, PIECE, 128):
                most = jnp.maximum(most, sums[:, j : j + 128])
            return most

        most = lax.fori_loop(0, 2 * Z * X, add, jnp.zeros((MINE, 128), jnp.float32))
        factor = jnp.max(most, axis=1, keepdims=True)
        same = lax.broadcasted_iota(jnp.int32, (MINE, MINE), 0) == lax.broadcasted_iota(
            jnp.int32, (MINE, MINE), 1
        )
        f0[...] = jnp.max(jnp.where(same, factor, 0.0), axis=0, keepdims=True)
        scale = 1.0 / factor

        def divide(i, _):
            here = lanes_at(i * PIECE, PIECE)
            o0[:, here] = (sums0[:, here] * scale).astype(jnp.bfloat16)
            return 0

        lax.fori_loop(0, 2 * Z * X, divide, 0)

    def block(m, dz, dx, first, size):
        return turned.at[m, rows_at(at(dz, dx) * MINE + first, size), :]

    def place_of(m, first, size, dz, dx):
        return outs[m].at[first : first + size, lanes_at(at(dz, dx) * ROWS, ROWS)]

    def straight(m, dz, dx):
        n = dz - 1 if dz else 2 + dx
        return remote(
            block(m, dz, dx, 0, MINE),
            place_of(m, 0, MINE, 0, 0),
            send.at[m, n],
            recv.at[m, n],
            dz,
            dx,
        )

    def number(dz, dx):
        return 3 * (dz - 1) + dx - 1

    def first_z(m, dz, dx):
        n = 6 + number(dz, dx)
        return remote(
            block(m, dz, dx, 0, HALF),
            rel_z.at[m, dz - 1, dx - 1],
            send.at[m, n],
            recv.at[m, n],
            dz,
            0,
        )

    def first_x(m, dz, dx):
        n = 15 + number(dz, dx)
        return remote(
            block(m, dz, dx, HALF, HALF),
            rel_x.at[m, dz - 1, dx - 1],
            send.at[m, n],
            recv.at[m, n],
            0,
            dx,
        )

    def then_x(m, dz, dx):
        n = 24 + number(dz, dx)
        return remote(
            rel_z.at[m, dz - 1, dx - 1],
            place_of(m, 0, HALF, -dz, 0),
            send.at[m, n],
            recv.at[m, n],
            0,
            dx,
        )

    def then_z(m, dz, dx):
        n = 33 + number(dz, dx)
        return remote(
            rel_x.at[m, dz - 1, dx - 1],
            place_of(m, HALF, HALF, 0, -dx),
            send.at[m, n],
            recv.at[m, n],
            dz,
            0,
        )

    sent, landing, owns = [], [[], [], []], []

    def hops_of(m):
        return [c(m, *d) for a, b in ROUNDS for c, d in ((first_z, (a, b)), (first_x, (b, a)))]

    def send_hops(m):
        sent.extend(start(hops_of(m)))

    def send_straight(m):
        copies = start([straight(m, *d) for a in STEPS for d in ((a, 0), (0, a))])
        sent.extend(copies)
        landing[m].extend(copies)
        own = pltpu.make_async_copy(
            block(m, 0, 0, 0, MINE), place_of(m, 0, MINE, 0, 0), own_sem.at[m]
        )
        own.start()
        owns.append(own)

    def relay(m):
        for a, b in (ROUNDS if m < 2 else LAST):
            first_x(m, a, b).wait_recv()
            first_z(m, b, a).wait_recv()
            sent.extend(start([then_z(m, a, b), then_x(m, b, a)]))
            landing[m].extend(sent[-2:])

    turn_first()
    pl.semaphore_wait(barrier, 6 + tp)
    at_first = hops_of(0)
    sent.extend(at_first)

    @pl.when(core == 1)
    def _():
        start(at_first)

    for d in range(1, TP):

        @pl.when(d <= tp)
        def _():
            pl.semaphore_signal(
                entered, 1, device_id={"tp": (tp + TP - d) % TP}, device_id_type=MESH
            )

    def share(part, s, r, n, **device):
        return pltpu.make_async_remote_copy(
            part, part, s.at[n], r.at[n], device_id=device, device_id_type=MESH
        )

    def gather(stage):
        if stage == 0:
            parts = gains.at[core, major, minor, y], own_low
            targets = [(d - 1, {"fsdp": at(d - core * d, core * d)}) for d in STEPS]
        elif stage == 1:
            lanes = lanes_at(X * major * PIECE, X * PIECE)
            parts = gains.at[core, major, :, y], lows.at[core, rows_at(16 * y, 16), lanes]
            targets = [(2 + d, {"fsdp": at(core * d, d - core * d)}) for d in STEPS]
        else:
            parts = gains.at[core, :, :, y], lows.at[core, rows_at(16 * y, 16), :]
            targets = [(5 + d, {"tp": (tp + d) % TP}) for d in range(1, TP)]
        sems = (gain_send, gain_recv), (low_send, low_recv)
        return start([share(p, *q, n, **t) for n, t in targets for p, q in zip(parts, sems)])

    merge(0)
    merge(1)
    small = [start(max_copies(0))]

    @pl.when(core == 0)
    def _():
        start(at_first)

    for c in extra:
        c.wait()
    gains[core, major, minor, y, :, 0:MINE] = adds[0] + adds[1]
    small.append(gather(0))
    send_straight(0)
    wait_recv(small[0])
    max_x[x] = largest(max_z)
    small.append(start(max_copies(1)))
    wait_recv(small[1])
    small.append(gather(1))
    relay(0)
    wait_recv(small[2])
    factor = largest(max_x)
    inverse[...] = 1.0 / factor
    for m in (0, 1):
        outputs = pltpu.roll(factor[m], (COLS - MINE * me) % COLS, 1)
        factors[1 + m][...] = outputs[:, :MINE]
    turn(0)
    send_hops(1)
    send_straight(1)
    wait_recv(small[3])

    @pl.when(tp < TP - 1)
    def _():
        pl.semaphore_wait(entered, TP - 1 - tp)

    small.append(gather(2))
    turn(1)
    send_hops(2)
    send_straight(2)
    wait_recv(landing[0])
    owns[0].wait()
    wait_recv(small[4])
    finish_first()
    relay(1)
    relay(2)
    lane = lax.broadcasted_iota(jnp.int32, (1, 128), 1)

    def pack(g, _):
        f = g // 2
        p, q, t = f // X, f % X, 2 * (g % 2)
        a, c = gains[0, q, p, t], gains[0, q, p, t + 1]
        b, d = gains[1, p, q, t], gains[1, p, q, t + 1]
        b, c, d = pltpu.roll(b, 96, 1), pltpu.roll(c, 64, 1), pltpu.roll(d, 32, 1)
        dense[pl.ds(3 * g, 1), :] = jnp.where(lane < 96, a, b)
        dense[pl.ds(3 * g + 1, 1), :] = jnp.where(lane < 64, b, c)
        dense[pl.ds(3 * g + 2, 1), :] = jnp.where(lane < 32, c, d)
        return 0

    lax.fori_loop(0, Z * X * TP // 4, pack, 0)
    norm[...] = dense[...].astype(jnp.bfloat16)
    for c in owns[1:]:
        c.wait()
    last = len(sent) - 2 * len(LAST)
    for c in (*sum(small, []), *sent[:last]):
        c.wait_send()
    wait_recv(landing[1] + landing[2])
    for c in sent[last:]:
        c.wait_send()


def write_out(*refs):
    copies = [
        pltpu.make_async_copy(a, b, refs[14].at[n])
        for n, (a, b) in enumerate(zip(refs[:7], refs[7:14]))
    ]
    for c in copies:
        c.start()
    for c in copies:
        c.wait()


def local(w0, l0, h0, w1, l1, h1, w2, l2, h2, train, step):
    f32, bf16 = jnp.float32, jnp.bfloat16
    vmem = pl.BlockSpec(memory_space=pltpu.VMEM)
    dma = pltpu.SemaphoreType.DMA
    gathered = pl.pallas_call(
        kernel,
        out_shape=[
            *[pltpu.VMEM((MINE, WHOLE), bf16)] * 3,
            *[pltpu.VMEM((1, MINE), f32)] * 3,
            pltpu.VMEM((WHOLE // 128, 128), bf16),
        ],
        in_specs=[pl.BlockSpec(memory_space=pltpu.HBM)] * 11,
        out_specs=[vmem] * 7,
        scratch_shapes=[
            pltpu.VMEM((3, ROWS, COLS), bf16),
            pltpu.VMEM((2, RANK, ROWS), bf16),
            pltpu.VMEM((3, RANK, COLS), bf16),
            pltpu.VMEM((2, ROWS, COLS), f32),
            pltpu.VMEM((MINE, WHOLE), f32),
            pltpu.VMEM((3, COLS, ROWS), bf16),
            pltpu.VMEM((3, 3, 3, HALF, ROWS), bf16),
            pltpu.VMEM((3, 3, 3, HALF, ROWS), bf16),
            pltpu.VMEM((Z, 2, 1, COLS), f32),
            pltpu.VMEM((X, 2, 1, COLS), f32),
            pltpu.VMEM((2, 1, COLS), f32),
            pltpu.VMEM((2, 1, MINE), f32),
            pltpu.VMEM((2, X, X, 4, 1, 128), f32),
            pltpu.VMEM((MINE, 128), f32),
            pltpu.VMEM((2, RANK, Z * X * PIECE), bf16),
            dma((14,)),
            dma((2, 3)),
            dma((2, 3)),
            dma((13,)),
            dma((13,)),
            dma((13,)),
            dma((13,)),
            dma((3, 42)),
            dma((3, 42)),
            dma((3,)),
            pltpu.SemaphoreType.REGULAR,
        ],
        compiler_params=pltpu.CompilerParams(
            collective_id=0, has_side_effects=True, vmem_limit_bytes=VMEM
        ),
        name="merge_and_spread",
    )(
        w0, l0.T, h0, w1, l1.T, h1, w2, l2.T, h2,
        train.reshape(1, MINE), step.reshape(1, MINE),
    )
    o0, o1, o2, f0, f1, f2, norm = pl.pallas_call(
        write_out,
        out_shape=[jax.ShapeDtypeStruct(a.shape, a.dtype) for a in gathered],
        in_specs=[pl.BlockSpec(memory_space=pl.ANY)] * 7,
        out_specs=[pl.BlockSpec(memory_space=pltpu.HBM)] * 7,
        scratch_shapes=[dma((7,))],
        compiler_params=pltpu.CompilerParams(vmem_limit_bytes=1024 * 1024),
        name="write_out",
    )(*gathered)
    return (
        o0.T, o1.T, o2.T,
        f0.reshape(MINE), f1.reshape(MINE), f2.reshape(MINE),
        norm.reshape(WHOLE),
    )


def solution(mesh):
    return jax.shard_map(
        local,
        mesh=mesh,
        in_specs=(
            *(P("fsdp", "tp"), P("fsdp", None), P(None, "tp")) * 3,
            P(("fsdp", "tp")),
            P(("fsdp", "tp")),
        ),
        out_specs=(*[P(None, ("tp", "fsdp"))] * 3, *[P(("tp", "fsdp"))] * 3, P()),
        check_vma=False,
    )
```
